32 devices in a mesh: tp: 4 (over z), pp: 8 (over y, x, core).
Axes of the slice: x: 2, y: 2, z: 4, core: 2. Of those that a mesh axis runs over, the one named last changes fastest.
Arguments:
- tokens: bfloat16 [8192, 8192], P('pp', 'tp'), may hold values from -60 to 60
- norm_gain: bfloat16 [8192], P('tp'), may hold values from 0.099609375 to 1.8984375
- weights_gen: bfloat16 [8, 1280, 8192], P('tp', None, 'pp'), may hold values from -2 to 2
- segment_ids: int32 [8, 1024], P('pp'), may hold values from 0 to 15, never falling along the last dimension, each value on 1 to 512 neighbouring positions
Outputs:
- weights_rows: bfloat16 [8, 1280, 8192], P('tp', 'pp')
- attended: bfloat16 [8192, 8192], P('pp', 'tp')
The draws below stay inside these ranges and needn't reach their ends.
Inputs may be any that keep to these rules, and one draw needn't show every extreme that they name: `segment_ids`: ids never fall along a block; every sequence has 1 to 512 tokens and lies in one block.
All inputs are finite; a program needn't handle non-finite values.
Results may differ from the reference program's by a relative error of at most 0.0075.
Values may be sent and summed in bfloat16 or wider, within the bound.
No kernel may reach another device: no remote copies, remote signals or barrier semaphores. Data moves between devices by JAX's collectives and lax.ppermute only.
A program may use at most 192 MiB of HBM per device.

```python
import math
import jax
import jax.numpy as jnp
import numpy as np
from jax import lax

D = 8192
HQ = 64
KVH = 8
DH = 128
TOK_DEV = 1024
GROUP = 8
QROWS = 1280
BLOCKS = 8
TOKENS = 8192
SEGS = 16


def draw_tokens(key, part):
    first = jax.random.fold_in(jax.random.fold_in(key, 11), 0)
    base = jax.random.truncated_normal(first, -6.0, 6.0, (TOKENS, D), jnp.float32)
    return jnp.clip(base, -60.0, 60.0).astype(jnp.bfloat16)


def draw_weights_gen(key, part):
    first = jax.random.fold_in(jax.random.fold_in(key, 23), 0)
    base = jax.random.truncated_normal(first, -6.0, 6.0, (KVH, QROWS, D), jnp.float32) / math.sqrt(D)
    return jnp.clip(base, -2.0, 2.0).astype(jnp.bfloat16)


def length_profile(count, total, limit, lean):
    portions = [(1 << 20) // math.isqrt(rank ** lean) + 1 for rank in range(2, count + 1)]
    rest, counts = total - limit - (count - 1), [1] * (count - 1)
    while rest > 0:
        candidates = [i for i in range(count - 1) if counts[i] < limit]
        whole, budget = sum([portions[i] for i in candidates]), rest
        for i in candidates:
            addition = min(limit - counts[i], max(1, budget * portions[i] // whole), rest)
            counts[i] = counts[i] + addition
            rest = rest - addition
    return np.array([limit] + counts)


def uneven_parts(rng, amount, total, limit, lean):
    if amount == 2:
        one = jax.random.randint(rng, (), max(1, total - limit), min(limit, total - 1) + 1)
        return jnp.stack([one, total - one])
    lengths = jnp.asarray(length_profile(amount, total, limit, lean), jnp.int32)
    pairs = (amount - 1) // 2
    donor, taker = lengths[1:1 + 2 * pairs:2], lengths[2:2 + 2 * pairs:2]
    margin = jnp.minimum(donor - 1, limit - taker)
    passed = jax.random.randint(jax.random.fold_in(rng, 1), (pairs,), 0, 1 << 20) % (margin + 1)
    lengths = lengths.at[1:1 + 2 * pairs:2].set(donor - passed).at[2:2 + 2 * pairs:2].set(taker + passed)
    return lengths[jax.random.permutation(jax.random.fold_in(rng, 2), amount)]


def setup_inputs(seed: int = 0) -> dict:
    splits = jax.random.split(jax.random.key(seed), 5)
    return {
        "tokens": draw_tokens(jax.random.fold_in(splits[4], 71), 0),
        "norm_gain": jnp.clip(1.0 + 0.18 * jax.random.normal(splits[1], (D,), jnp.float32), 0.099609375, 1.8984375).astype(jnp.bfloat16),
        "weights_gen": draw_weights_gen(jax.random.fold_in(splits[4], 71), 0),
        "segment_ids": jax.vmap(lambda own: jnp.searchsorted(jnp.cumsum(uneven_parts(own, SEGS, TOK_DEV, TOK_DEV // 2, 1)), jnp.arange(TOK_DEV), side="right"))(jax.random.split(splits[3], BLOCKS)).reshape((BLOCKS, TOK_DEV)).astype(jnp.int32),
    }


rope_base = 500000.0

def rotary(values, positions):
    half = values.shape[-1] // 2
    freq = jnp.exp(jnp.arange(half, dtype=jnp.float32) * (-2.0 * math.log(rope_base) / values.shape[-1]))
    angle = positions.astype(jnp.float32)[:, None] * freq[None, :]
    cosine = jnp.cos(angle)
    sine = jnp.sin(angle)
    extra = values.ndim - 2
    cosine = cosine.reshape(cosine.shape[:1] + (1,) * extra + cosine.shape[1:])
    sine = sine.reshape(sine.shape[:1] + (1,) * extra + sine.shape[1:])
    first = values[..., :half]
    second = values[..., half:]
    return jnp.concatenate([first * cosine - second * sine, second * cosine + first * sine], axis=-1)

def block_positions(seg):
    count = seg.shape[0]
    start = lax.optimization_barrier(jnp.sum((seg[None, :] < seg[:, None]).astype(jnp.int32), axis=1))
    return jnp.arange(count, dtype=jnp.int32) - start

def attend_block(query, key, value, seg):
    count = seg.shape[0]
    score = jnp.einsum('tgjd,sgd->gjts', query.astype(jnp.float32), key.astype(jnp.float32)) * (1.0 / math.sqrt(DH))
    order = jnp.arange(count, dtype=jnp.int32)
    allowed = (seg[:, None] == seg[None, :]) & (order[:, None] >= order[None, :])
    score = jnp.where(allowed[None, None], score, -1e+30)
    top = lax.optimization_barrier(jnp.max(score, axis=-1, keepdims=True))
    expo = jnp.where(allowed[None, None], jnp.exp(score - top), 0.0)
    prob = (expo / lax.optimization_barrier(jnp.sum(expo, axis=-1, keepdims=True))).astype(jnp.bfloat16)
    out = jnp.einsum('gjts,sgd->tgjd', prob.astype(jnp.float32), value.astype(jnp.float32))
    return out.astype(jnp.bfloat16).reshape(count, -1)

def reference(tokens, norm_gain, weights_gen, segment_ids):
    floats = tokens.astype(jnp.float32)
    square = lax.optimization_barrier(jnp.mean(floats * floats, axis=-1, keepdims=True))
    normed = (floats * lax.rsqrt(square + 1e-05) * norm_gain.astype(jnp.float32)).astype(jnp.bfloat16)
    flat = weights_gen.reshape(KVH * QROWS, D)
    mixed = jnp.dot(normed, flat.T, preferred_element_type=jnp.float32)
    mixed = mixed.reshape(TOKENS, KVH, GROUP + 2, DH)
    positions = jax.vmap(block_positions)(segment_ids).reshape(TOKENS)
    query = rotary(mixed[:, :, :GROUP, :], positions).astype(jnp.bfloat16)
    key = rotary(mixed[:, :, GROUP, :], positions).astype(jnp.bfloat16)
    value = mixed[:, :, GROUP + 1, :].astype(jnp.bfloat16)
    query = query.reshape(BLOCKS, TOK_DEV, KVH, GROUP, DH)
    key = key.reshape(BLOCKS, TOK_DEV, KVH, DH)
    value = value.reshape(BLOCKS, TOK_DEV, KVH, DH)

    def one_block(items):
        return attend_block(items[0], items[1], items[2], items[3])
    attended = lax.map(one_block, (query, key, value, segment_ids))
    return (weights_gen, attended.reshape(TOKENS, HQ * DH))
```

```python
import functools
import math

import jax
import jax.numpy as jnp
from jax import lax
from jax.experimental import pallas as pl
from jax.experimental.pallas import tpu as pltpu
from jax.sharding import PartitionSpec as P

DH = 128
GROUP = 8
SPAN = 512
PAIR = 2 * DH
CHUNKS = 4
BF16 = jnp.bfloat16
F32 = jnp.float32

rope_base = 500000.0


NT = (((1,), (1,)), ((), ()))
NN = (((1,), (0,)), ((), ()))


def dot(a, b, dims):
    return lax.dot_general(a, b, dims, preferred_element_type=F32)


def params(mib=56):
    return pltpu.CompilerParams(vmem_limit_bytes=mib << 20)


def any_spec():
    return pl.BlockSpec(memory_space=pl.ANY)


def normalise(x_ref, inv_ref, gain, rows, start, put):
    step = min(rows, 64)

    @pl.loop(0, rows // step)
    def _(i):
        r = pl.multiple_of(i * step, step)
        x = x_ref[pl.ds(r, step), :].astype(F32)
        y = x * inv_ref[pl.ds(start + r, step), :] * gain
        put(start + r, step, y.astype(BF16))


def place_kernel(count, old, where_ref, *refs):
    ins = refs[:count]
    out, buf, sem_in, sem_out = refs[count + old :]
    part = ins[0].shape[0]

    def get(i):
        return pltpu.make_async_copy(ins[i], buf.at[i], sem_in.at[i])

    def put(i):
        at = out.at[where_ref[i // 2], pl.ds((i % 2) * part, part), :]
        return pltpu.make_async_copy(buf.at[i], at, sem_out.at[i])

    for i in range(count):
        get(i).start()
    for i in range(count):
        get(i).wait()
        put(i).start()
    for i in range(count):
        put(i).wait()


def place(whole, where, halves, slices):
    count = len(halves)
    part, width = halves[0].shape
    old = 0 if whole is None else 1
    grid = pltpu.PrefetchScalarGridSpec(
        num_scalar_prefetch=1,
        grid=(1,),
        in_specs=[any_spec()] * (count + old),
        out_specs=any_spec(),
        scratch_shapes=[
            pltpu.VMEM((count, part, width), BF16),
            pltpu.SemaphoreType.DMA((count,)),
            pltpu.SemaphoreType.DMA((count,)),
        ],
    )
    size = count * part * width * 2
    return pl.pallas_call(
        functools.partial(place_kernel, count, old),
        grid_spec=grid,
        out_shape=jax.ShapeDtypeStruct((slices, 2 * part, width), BF16),
        input_output_aliases={count + 1: 0} if old else {},
        compiler_params=params(),
        cost_estimate=pl.CostEstimate(flops=size * 100, bytes_accessed=2 * size, transcendentals=0),
        name="place",
    )(where, *halves, *([whole] if old else []))


def rows_kernel(me_ref, w_ref, o_ref):
    o_ref[0] = w_ref[0]


def take_rows(whole, me, groups, slices):
    rows = whole.shape[1] // groups // slices
    width = whole.shape[2]
    grid = pltpu.PrefetchScalarGridSpec(
        num_scalar_prefetch=1,
        grid=(groups, slices),
        in_specs=[pl.BlockSpec((1, rows, width), lambda g, p, me: (p, g * slices + me[0], 0))],
        out_specs=pl.BlockSpec((1, rows, width), lambda g, p, me: (g, 0, p)),
    )
    size = groups * rows * slices * width * 2
    return pl.pallas_call(
        rows_kernel,
        grid_spec=grid,
        out_shape=jax.ShapeDtypeStruct((groups, rows, slices * width), BF16),
        compiler_params=params(),
        cost_estimate=pl.CostEstimate(flops=size * 100, bytes_accessed=2 * size, transcendentals=0),
        name="take_rows",
    )(me, whole)


def early_kernel(steps, chunks, per, which_ref, *refs):
    pieces = refs[: 1 + (steps - 1) * chunks]
    refs = refs[len(pieces) :]
    inv_ref, gain_ref = refs[:2]
    weights = refs[2 : 2 + steps]
    acc_ref, xn = refs[2 + steps :]
    count = acc_ref.shape[0]
    width = xn.shape[2]
    f2 = width // per

    @pl.when(pl.program_id(0) == 0)
    def _():
        at = 0
        for k in range(steps):
            gain = gain_ref[k : k + 1, :]
            for c in range(1 if k == 0 else chunks):
                ref = pieces[at]
                at += 1
                rows = ref.shape[0]

                def put(r, n, y, k=k):
                    xn[k, pl.ds(r, n), :] = y

                normalise(ref, inv_ref, gain, rows, c * rows, put)

    block = min(count, 512)

    @pl.loop(0, count // block)
    def _(i):
        r = pl.ds(pl.multiple_of(i * block, block), block)
        total = None
        for k in range(steps):
            for j in range(per):
                part = dot(xn[k, r, j * f2 : (j + 1) * f2], weights[k][0, j], NT)
                total = part if total is None else total + part
        acc_ref[r, :] = total


def early(which, pieces, inv, gains, whole, per):
    count, width = pieces[0].shape
    parts = gains.shape[0]
    steps = parts - 1
    chunks = (len(pieces) - 1) // max(steps - 1, 1)
    rows = whole.shape[1]
    w4 = whole.reshape(parts, per, rows, whole.shape[2])

    def once(shape):
        return pl.BlockSpec(shape, lambda n, f: (0,) * len(shape), pipeline_mode=pl.Buffered(1))

    def wspec(k):
        return pl.BlockSpec((1, per, PAIR, whole.shape[2]), lambda n, f: (f[k], 0, n, 0))

    grid = pltpu.PrefetchScalarGridSpec(
        num_scalar_prefetch=1,
        grid=(rows // PAIR,),
        in_specs=[once(p.shape) for p in pieces]
        + [once(inv.shape), once(gains.shape)]
        + [wspec(k) for k in range(steps)],
        out_specs=pl.BlockSpec((count, PAIR), lambda n, f: (0, n)),
        scratch_shapes=[pltpu.VMEM((steps, count, width), BF16)],
    )
    return pl.pallas_call(
        functools.partial(early_kernel, steps, chunks, per),
        grid_spec=grid,
        out_shape=jax.ShapeDtypeStruct((count, rows), F32),
        compiler_params=params(60),
        cost_estimate=pl.CostEstimate(
            flops=2 * count * width * steps * rows,
            bytes_accessed=steps * width * (rows + count) * 2 + count * rows * 4,
            transcendentals=0,
        ),
        name="early",
    )(which, *pieces, inv, gains, *([w4] * steps))


def late_kernel(c, hist, per, aliased, which_ref, x_ref, inv_ref, gain_ref, w_ref, acc_ref, cos_ref, sin_ref, begin_ref, *refs):
    past = refs[:hist]
    out_ref, kv_ref, xn, bias, queries = refs[hist + aliased :]
    rows, width = x_ref.shape
    f2 = width // per
    n = pl.program_id(0)
    i = n % (GROUP // 2 + 1)
    wide = (hist + 1) * rows

    @pl.when(n == 0)
    def _():
        last = gain_ref.shape[0] - 1
        gain = gain_ref[last : last + 1, :]

        def put(r, m, y):
            xn[pl.ds(r, m), :] = y

        normalise(x_ref, inv_ref, gain, rows, 0, put)
        row = c * rows + lax.broadcasted_iota(jnp.int32, (rows, wide), 0)
        col = (c - hist) * rows + lax.broadcasted_iota(jnp.int32, (rows, wide), 1)
        bias[...] = jnp.where((col <= row) & (col >= begin_ref[...]), 0.0, -1e30)

    total = acc_ref[...]
    for j in range(per):
        total = total + dot(xn[:, j * f2 : (j + 1) * f2], w_ref[0, j], NT)

    def rotary(u):
        return (u * cos_ref[...] + pltpu.roll(u, DH // 2, 1) * sin_ref[...]).astype(BF16)

    first = rotary(total[:, :DH])

    @pl.when(i == 0)
    def _():
        kv_ref[:, :DH] = first
        kv_ref[:, DH:] = total[:, DH:].astype(BF16)

    @pl.when(i != 0)
    def _():
        queries[:, :DH] = first
        queries[:, DH:] = rotary(total[:, DH:])
        for h in range(2):
            q = queries[:, h * DH : (h + 1) * DH]
            scores = []
            for p in range(hist + 1):
                src = past[p] if p < hist else kv_ref
                s = dot(q, src[:, :DH], NT) * (1.0 / math.sqrt(DH))
                scores.append(s + bias[:, p * rows : (p + 1) * rows])
            top = scores[0].max(axis=1, keepdims=True)
            for s in scores[1:]:
                top = jnp.maximum(top, s.max(axis=1, keepdims=True))
            expo = [jnp.exp(s - top) for s in scores]
            norm = expo[0].sum(axis=1, keepdims=True)
            for e in expo[1:]:
                norm = norm + e.sum(axis=1, keepdims=True)
            scale = 1.0 / norm
            out = None
            for p in range(hist + 1):
                src = past[p] if p < hist else kv_ref
                part = dot((expo[p] * scale).astype(BF16), src[:, DH:], NN)
                out = part if out is None else out + part
            out_ref[:, h * DH : (h + 1) * DH] = out.astype(BF16)


def late(c, which, x, inv, gains, whole, per, acc, cos, sin, begin, past, out):
    rows, width = x.shape
    count, cols = acc.shape
    parts = gains.shape[0]
    w4 = whole.reshape(parts, per, cols, whole.shape[2])
    hist = len(past)
    blocks = GROUP // 2 + 1
    groups = cols // PAIR // blocks
    aliased = 0 if out is None else 1

    def col(n):
        return n // blocks * blocks + (n % blocks + blocks - 1) % blocks

    def ocol(n):
        return n // blocks * (blocks - 1) + jnp.maximum(n % blocks, 1) - 1

    grid = pltpu.PrefetchScalarGridSpec(
        num_scalar_prefetch=1,
        grid=(groups * blocks,),
        in_specs=[
            pl.BlockSpec((rows, width), lambda n, f: (0, 0)),
            pl.BlockSpec((rows, 1), lambda n, f: (c, 0)),
            pl.BlockSpec(gains.shape, lambda n, f: (0, 0)),
            pl.BlockSpec((1, per, PAIR, whole.shape[2]), lambda n, f: (f[0], 0, col(n), 0)),
            pl.BlockSpec((rows, PAIR), lambda n, f: (c, col(n))),
            pl.BlockSpec((rows, DH), lambda n, f: (c, 0)),
            pl.BlockSpec((rows, DH), lambda n, f: (c, 0)),
            pl.BlockSpec((rows, 1), lambda n, f: (c, 0)),
        ]
        + [pl.BlockSpec((rows, PAIR), lambda n, f: (0, n // blocks))] * hist
        + [any_spec()] * aliased,
        out_specs=[
            pl.BlockSpec((rows, PAIR), lambda n, f: (c, ocol(n))),
            pl.BlockSpec((rows, PAIR), lambda n, f: (0, n // blocks)),
        ],
        scratch_shapes=[
            pltpu.VMEM((rows, width), BF16),
            pltpu.VMEM((rows, (hist + 1) * rows), F32),
            pltpu.VMEM((rows, PAIR), BF16),
        ],
    )
    heads = groups * GROUP
    return pl.pallas_call(
        functools.partial(late_kernel, c, hist, per, aliased),
        grid_spec=grid,
        out_shape=(
            jax.ShapeDtypeStruct((count, heads * DH), BF16),
            jax.ShapeDtypeStruct((rows, groups * PAIR), BF16),
        ),
        input_output_aliases={9 + hist: 0} if aliased else {},
        compiler_params=params(),
        cost_estimate=pl.CostEstimate(
            flops=2 * rows * width * cols + 4 * rows * rows * (hist + 1) * DH * heads,
            bytes_accessed=width * cols * 2 + rows * cols * 4 + rows * heads * DH * 2,
            transcendentals=rows * rows * (hist + 1) * heads,
        ),
        name="late",
    )(which, x, inv, gains, w4, acc, cos, sin, begin, *past, *([out] if aliased else []))


def shards(axes, tokens, norm_gain, weights_gen, segment_ids):
    tp, pp = axes["tp"], axes["pp"]
    count, width = tokens.shape
    groups, qrows, f2 = weights_gen.shape
    per = width // f2
    chunks = CHUNKS
    rows = count // chunks
    me = lax.axis_index("pp")
    z = lax.axis_index("tp")

    ring = [(i, (i - 1) % tp) for i in range(tp)]
    step = [tokens[c * rows : (c + 1) * rows] for c in range(chunks)]
    got = []
    for k in range(1, tp):
        step = [lax.ppermute(s, "tp", ring) for s in step]
        got.append(step)

    flat = weights_gen.reshape(groups * qrows, f2)
    part = flat.shape[0] // 2

    def swap(x, mask):
        return lax.ppermute(x, "pp", [(i, i ^ mask) for i in range(pp)])

    slices = {0: [flat[:part], flat[part:]]}
    order = sorted(range(2, pp, 2), key=lambda m: (bin(m).count("1"), m))
    for m in order:
        bits = [1 << b for b in range(pp.bit_length()) if m >> b & 1]
        via = [bits[0], bits[-1]]
        slices[m] = [swap(slices[m ^ via[h]][h], via[h]) for h in range(2)]
    for m in [0] + order:
        slices[m | 1] = [swap(s, 1) for s in slices[m]]

    floats = tokens.astype(F32)
    small = jnp.concatenate([jnp.sum(floats * floats, axis=1), norm_gain.astype(F32)])
    small = small.reshape(-1, 128)
    smalls = [small]
    for k in range(1, tp):
        smalls.append(lax.ppermute(small, "tp", [(i, (i - k) % tp) for i in range(tp)]))
    smalls = [s.reshape(-1) for s in smalls]
    square = sum(s[:count] for s in smalls) / (tp * width)
    inv = lax.rsqrt(square + 1e-05)[:, None]
    gains = jnp.stack([s[count:] for s in smalls])
    which = (z + jnp.arange(tp, dtype=jnp.int32)) % tp

    seg = segment_ids[0]
    begin = jnp.sum((seg[None, :] < seg[:, None]).astype(jnp.int32), axis=1)
    positions = jnp.arange(count, dtype=jnp.int32) - begin
    half = DH // 2
    freq = jnp.exp(jnp.arange(half, dtype=F32) * (-2.0 * math.log(rope_base) / DH))
    angle = positions.astype(F32)[:, None] * freq[None, :]
    cosine, sine = jnp.cos(angle), jnp.sin(angle)
    cos = jnp.concatenate([cosine, cosine], axis=1)
    sin = jnp.concatenate([-sine, sine], axis=1)

    stages = [[m for m in [0] + order if bin(m).count("1") == n] for n in range(pp.bit_length())]
    whole = None
    for stage in stages:
        if not stage:
            continue
        masks = [m | b for m in stage for b in (0, 1)]
        halves = [h for m in masks for h in slices[m]]
        where = me ^ jnp.array(masks, jnp.int32)
        whole = place(whole, where.astype(jnp.int32), halves, pp)
    weights_rows = take_rows(whole, me.astype(jnp.int32)[None], groups, pp)
    whole, weights_rows = lax.optimization_barrier((whole, weights_rows))

    pieces = [tokens] + [s for k in range(tp - 2) for s in got[k]]
    acc = early(which, pieces, inv, gains, whole, per)

    out, past = None, []
    hist = -(-(SPAN - 1) // rows)
    for c in range(chunks):
        out, kv = late(
            c, which[tp - 1 :], got[-1][c], inv, gains, whole, per, acc, cos, sin,
            begin[:, None], past[-hist:], out,
        )
        past.append(kv)
    return weights_rows, out


def solution(mesh):
    in_specs = (P("pp", "tp"), P("tp"), P("tp", None, "pp"), P("pp", None))
    out_specs = (P("tp", "pp", None), P("pp", "tp"))
    body = functools.partial(shards, dict(mesh.shape))
    return jax.shard_map(body, mesh=mesh, in_specs=in_specs, out_specs=out_specs, check_vma=False)
```

```python
import functools
import math

import jax
import jax.numpy as jnp
from jax import lax
from jax.experimental import pallas as pl
from jax.experimental.pallas import tpu as pltpu
from jax.sharding import PartitionSpec as P


DH = 128
GROUP = 8
SPAN = 512
PAIR = 2 * DH
CHUNKS = 4
BF16 = jnp.bfloat16
F32 = jnp.float32

rope_base = 500000.0


NT = (((1,), (1,)), ((), ()))
NN = (((1,), (0,)), ((), ()))


def dot(a, b, dims):
    return lax.dot_general(a, b, dims, preferred_element_type=F32)


def params(mib=56):
    return pltpu.CompilerParams(vmem_limit_bytes=mib << 20)


def any_spec():
    return pl.BlockSpec(memory_space=pl.ANY)


def normalise(x_ref, inv_ref, gain, rows, start, put):
    step = min(rows, 16)

    @pl.loop(0, rows // step, unroll=4)
    def _(i):
        r = pl.multiple_of(i * step, step)
        x = x_ref[pl.ds(r, step), :].astype(F32)
        y = x * inv_ref[pl.ds(start + r, step), :] * gain
        put(start + r, step, y.astype(BF16))


def place_kernel(pieces, old, groups, slices, where_ref, *refs):
    count = len(pieces)
    ins = refs[:count]
    out, rows_out, buf, sem_in, sem_out, sem_rows = refs[count + 2 * old :]
    width = out.shape[2]
    own = out.shape[1] // groups // slices
    me = where_ref[0]
    spots = []
    used = 0
    for which, first, size in pieces:
        spots.append(pl.ds(used, size))
        used += size

    def get(i):
        return pltpu.make_async_copy(ins[i], buf.at[spots[i]], sem_in.at[i])

    def put(i):
        which, first, size = pieces[i]
        at = out.at[where_ref[1 + which], pl.ds(first, size), :]
        return pltpu.make_async_copy(buf.at[spots[i]], at, sem_out.at[i])

    def each(i, act):
        which, first, size = pieces[i]
        col = pl.multiple_of(where_ref[1 + which] * width, width)
        for g in range(groups):
            low, high = g * own * slices, (g + 1) * own * slices
            if high <= first or low >= first + size:
                continue
            at = low + me * own - first

            def go(at=at, col=col, g=g):
                src = buf.at[pl.ds(pl.multiple_of(spots[i].start + at, own), own), :]
                act(pltpu.make_async_copy(src, rows_out.at[g, :, pl.ds(col, width)], sem_rows.at[i, g]))

            if first <= low and high <= first + size:
                go()
            else:
                pl.when((at >= 0) & (at < size))(go)

    for i in range(count):
        get(i).start()
    for i in range(count):
        get(i).wait()
        put(i).start()
        each(i, lambda copy: copy.start())
    for i in range(count):
        put(i).wait()
        each(i, lambda copy: copy.wait())


def place(state, where, items, rows, groups, slices):
    arrays = [x for _, _, x in items]
    pieces = [(which, first, x.shape[0]) for which, first, x in items]
    width = arrays[0].shape[1]
    count = len(arrays)
    total = sum(size for _, _, size in pieces)
    old = 0 if state is None else 1
    grid = pltpu.PrefetchScalarGridSpec(
        num_scalar_prefetch=1,
        grid=(1,),
        in_specs=[any_spec()] * (count + 2 * old),
        out_specs=[any_spec()] * 2,
        scratch_shapes=[
            pltpu.VMEM((total, width), BF16),
            pltpu.SemaphoreType.DMA((count,)),
            pltpu.SemaphoreType.DMA((count,)),
            pltpu.SemaphoreType.DMA((count, groups)),
        ],
    )
    size = total * width * 2
    return pl.pallas_call(
        functools.partial(place_kernel, pieces, old, groups, slices),
        grid_spec=grid,
        out_shape=(
            jax.ShapeDtypeStruct((slices, rows, width), BF16),
            jax.ShapeDtypeStruct((groups, rows // groups // slices, slices * width), BF16),
        ),
        input_output_aliases={count + 1: 0, count + 2: 1} if old else {},
        compiler_params=params(),
        cost_estimate=pl.CostEstimate(flops=size * 100, bytes_accessed=2 * size, transcendentals=0),
        name="place",
    )(where, *arrays, *(state if old else ()))


def prep_kernel(k, x_ref, inv_ref, gain_ref, *refs):
    o_ref = refs[-1]

    def put(r, n, y):
        o_ref[0, pl.ds(r, n), :] = y

    normalise(x_ref, inv_ref, gain_ref[k : k + 1, :], x_ref.shape[0], 0, put)


def prep(k, start, x, inv, gains, out):
    rows, width = x.shape
    block = min(rows, 256)
    at = start // block
    extra = 0 if out is None else 1
    return pl.pallas_call(
        functools.partial(prep_kernel, k),
        grid=(rows // block,),
        in_specs=[
            pl.BlockSpec((block, width), lambda i: (i, 0)),
            pl.BlockSpec((block, 1), lambda i: (at + i, 0)),
            pl.BlockSpec(gains.shape, lambda i: (0, 0)),
        ]
        + [any_spec()] * extra,
        out_specs=pl.BlockSpec((1, block, width), lambda i: (k, at + i, 0)),
        out_shape=jax.ShapeDtypeStruct((gains.shape[0] - 1, inv.shape[0], width), BF16),
        input_output_aliases={3: 0} if extra else {},
        compiler_params=params(),
        cost_estimate=pl.CostEstimate(flops=rows * width * 100, bytes_accessed=rows * width * 4, transcendentals=0),
        name="prep",
    )(x, inv, gains, *([out] if extra else []))


def early_kernel(units, per, old, which_ref, x_hbm, *refs):
    weights = refs[:units]
    acc_ref, xs, sems = refs[-3:]
    _, count, width = xs.shape
    f2 = width // per
    block = min(count, 512)
    first = pl.program_id(0) == 0

    def get(u, i):
        at = pl.ds(pl.multiple_of(i * block, block), block)
        return pltpu.make_async_copy(x_hbm.at[which_ref[u], at], xs.at[u, at], sems.at[u, i])

    @pl.when(first)
    def _():
        for i in range(count // block):
            for u in range(units):
                get(u, i).start()

    @pl.loop(0, count // block)
    def _(i):
        r = pl.ds(pl.multiple_of(i * block, block), block)

        @pl.when(first)
        def _():
            for u in range(units):
                get(u, i).wait()

        if old:
            acc_ref[:, r] = refs[units][:, r]
        else:
            acc_ref[:, r] = jnp.zeros((acc_ref.shape[0], block), F32)
        for u in range(units):

            @pl.when(which_ref[2 * units + u] != 0)
            def _():
                total = acc_ref[:, r]
                for j in range(per):
                    total = total + dot(weights[u][0, j], xs[u, r, j * f2 : (j + 1) * f2], NT)
                acc_ref[:, r] = total


def early(units, which, xs, whole, per, acc):
    _, count, width = xs.shape
    rows = whole.shape[1]
    w4 = whole.reshape(-1, per, rows, whole.shape[2])
    block = 2 * PAIR if rows % (2 * PAIR) == 0 else PAIR
    old = 0 if acc is None else 1

    def wspec(u):
        return pl.BlockSpec((1, per, block, whole.shape[2]), lambda n, f: (f[units + u], 0, n, 0))

    aspec = pl.BlockSpec((block, count), lambda n, f: (n, 0))
    grid = pltpu.PrefetchScalarGridSpec(
        num_scalar_prefetch=1,
        grid=(rows // block,),
        in_specs=[any_spec()] + [wspec(u) for u in range(units)] + [aspec] * old,
        out_specs=aspec,
        scratch_shapes=[
            pltpu.VMEM((units, count, width), BF16),
            pltpu.SemaphoreType.DMA((units, count // min(count, 512))),
        ],
    )
    return pl.pallas_call(
        functools.partial(early_kernel, units, per, old),
        grid_spec=grid,
        out_shape=jax.ShapeDtypeStruct((rows, count), F32),
        input_output_aliases={2 + units: 0} if old else {},
        compiler_params=params(60),
        cost_estimate=pl.CostEstimate(
            flops=2 * count * width * units * rows,
            bytes_accessed=units * width * (rows + count) * 2 + count * rows * 4 * (1 + old),
            transcendentals=0,
        ),
        name="early",
    )(which, xs, *([w4] * units), *([acc] if old else []))


def late_kernel(start, sizes, per, groups, aliased, which_ref, inv_ref, gain_ref, cos_ref, sin_ref, begin_ref, *refs):
    hist = len(sizes)
    keys = refs[:hist]
    values = refs[hist : 2 * hist]
    x_hbm, w_hbm, acc_hbm = refs[2 * hist : 2 * hist + 3]
    out_ref, k_ref, v_ref, x_ref, w_ref, acc_ref, xn, bias, sems = refs[2 * hist + 3 + aliased :]
    rows, width = x_ref.shape
    f2 = width // per
    half = DH // 2
    blocks = GROUP // 2 + 1
    span = blocks * PAIR
    before = sum(sizes)
    wide = before + rows
    edges = [sum(sizes[:p]) for p in range(hist + 1)] + [wide]

    def get_x():
        return pltpu.make_async_copy(x_hbm, x_ref, sems.at[0])

    def get_acc(g):
        at = pl.ds(pl.multiple_of(g * span, PAIR), span)
        src = acc_hbm.at[at, pl.ds(start, rows)]
        return pltpu.make_async_copy(src, acc_ref.at[at], sems.at[1 + g])

    def get_w(g, j):
        at = pl.ds(pl.multiple_of(g * span, PAIR), span)
        src = w_hbm.at[which_ref[0], j, at]
        return pltpu.make_async_copy(src, w_ref.at[j, at], sems.at[1 + groups + g * per + j])

    get_x().start()
    for g in range(groups):
        for j in range(per):
            get_w(g, j).start()
        get_acc(g).start()

    key = start - before + lax.broadcasted_iota(jnp.int32, (wide, rows), 0)
    tok = start + lax.broadcasted_iota(jnp.int32, (wide, rows), 1)
    bias[...] = jnp.where((key <= tok) & (key >= begin_ref[...]), 0.0, -1e30)
    last = gain_ref.shape[0] - 1

    def put(r, m, y):
        xn[pl.ds(r, m), :] = y

    get_x().wait()
    normalise(x_ref, inv_ref, gain_ref[last : last + 1, :], rows, 0, put)

    def rotary(u):
        a, b = u[:half], u[half:]
        c, s = cos_ref[...], sin_ref[...]
        return jnp.concatenate([a * c - b * s, b * c + a * s], axis=0)

    def project(at):
        total = acc_ref[at, :]
        for j in range(per):
            total = total + dot(w_ref[j, at, :], xn[:, j * f2 : (j + 1) * f2], NT)
        return total

    @pl.loop(0, groups)
    def _(g):
        for j in range(per):
            get_w(g, j).wait()
        get_acc(g).wait()
        base = g * span
        total = project(pl.ds(pl.multiple_of(base + (blocks - 1) * PAIR, PAIR), PAIR))
        k_ref[g] = rotary(total[:DH]).T.astype(BF16)
        v_ref[g] = total[DH:].astype(BF16)

        for i in range(blocks - 1):
            total = project(pl.ds(pl.multiple_of(base + i * PAIR, PAIR), PAIR))
            for h in range(2):
                q = rotary(total[h * DH : (h + 1) * DH]).astype(BF16)
                scores = []
                for p in range(hist + 1):
                    src = keys[p] if p < hist else k_ref
                    s = dot(src[g], q, NN) * (math.log2(math.e) / math.sqrt(DH))
                    scores.append(s + bias[edges[p] : edges[p + 1], :])
                top = scores[0].max(axis=0, keepdims=True)
                for s in scores[1:]:
                    top = jnp.maximum(top, s.max(axis=0, keepdims=True))
                expo = [jnp.exp2(s - top) for s in scores]
                norm = expo[0].sum(axis=0, keepdims=True)
                for e in expo[1:]:
                    norm = norm + e.sum(axis=0, keepdims=True)
                scale = 1.0 / norm
                out = None
                for p in range(hist + 1):
                    src = values[p] if p < hist else v_ref
                    part = dot(src[g], expo[p].astype(BF16), NN)
                    out = part if out is None else out + part
                at = pl.multiple_of((g * (blocks - 1) + i) * PAIR + h * DH, DH)
                out_ref[:, pl.ds(at, DH)] = (out * scale).T.astype(BF16)


def late(start, which, x, inv, gains, whole, per, acc, cos, sin, begin, past, out):
    rows, width = x.shape
    cols, count = acc.shape
    c = start // rows
    w4 = whole.reshape(-1, per, cols, whole.shape[2])
    sizes = tuple(k.shape[1] for k, _ in past)
    groups = cols // DH // (GROUP + 2)
    heads = groups * GROUP
    aliased = 0 if out is None else 1
    wide = sum(sizes) + rows

    grid = pltpu.PrefetchScalarGridSpec(
        num_scalar_prefetch=1,
        grid=(1,),
        in_specs=[
            pl.BlockSpec((rows, 1), lambda n, f: (c, 0)),
            pl.BlockSpec(gains.shape, lambda n, f: (0, 0)),
            pl.BlockSpec((DH // 2, rows), lambda n, f: (0, c)),
            pl.BlockSpec((DH // 2, rows), lambda n, f: (0, c)),
            pl.BlockSpec((1, rows), lambda n, f: (0, c)),
        ]
        + [pl.BlockSpec((groups, r, DH), lambda n, f: (0, 0, 0)) for r in sizes]
        + [pl.BlockSpec((groups, DH, r), lambda n, f: (0, 0, 0)) for r in sizes]
        + [any_spec()] * (3 + aliased),
        out_specs=[
            pl.BlockSpec((rows, heads * DH), lambda n, f: (c, 0)),
            pl.BlockSpec((groups, rows, DH), lambda n, f: (0, 0, 0)),
            pl.BlockSpec((groups, DH, rows), lambda n, f: (0, 0, 0)),
        ],
        scratch_shapes=[
            pltpu.VMEM((rows, width), BF16),
            pltpu.VMEM((per, cols, whole.shape[2]), BF16),
            pltpu.VMEM((cols, rows), F32),
            pltpu.VMEM((rows, width), BF16),
            pltpu.VMEM((wide, rows), F32),
            pltpu.SemaphoreType.DMA((1 + groups + groups * per,)),
        ],
    )
    return pl.pallas_call(
        functools.partial(late_kernel, start, sizes, per, groups, aliased),
        grid_spec=grid,
        out_shape=(
            jax.ShapeDtypeStruct((count, heads * DH), BF16),
            jax.ShapeDtypeStruct((groups, rows, DH), BF16),
            jax.ShapeDtypeStruct((groups, DH, rows), BF16),
        ),
        input_output_aliases={9 + 2 * len(sizes): 0} if aliased else {},
        compiler_params=params(),
        cost_estimate=pl.CostEstimate(
            flops=2 * rows * width * cols + 4 * rows * wide * DH * heads,
            bytes_accessed=width * cols * 2 + rows * cols * 4 + rows * heads * DH * 2,
            transcendentals=rows * wide * heads,
        ),
        name="late",
    )(
        which, inv, gains, cos, sin, begin,
        *[k for k, _ in past], *[v for _, v in past], x, w4, acc, *([out] if aliased else []),
    )


def cut_kernel(first, size, x_hbm, o_ref, sem):
    copy = pltpu.make_async_copy(x_hbm.at[pl.ds(first, size)], o_ref, sem)
    copy.start()
    copy.wait()


def cut(x, first, size):
    return pl.pallas_call(
        functools.partial(cut_kernel, first, size),
        in_specs=[any_spec()],
        out_specs=pl.BlockSpec(memory_space=pltpu.VMEM),
        out_shape=jax.ShapeDtypeStruct((size, x.shape[1]), x.dtype),
        scratch_shapes=[pltpu.SemaphoreType.DMA],
        compiler_params=params(60),
        name="cut",
    )(x)


def shards(axes, tokens, norm_gain, weights_gen, segment_ids):
    return layer(axes, tokens, norm_gain, weights_gen, segment_ids)


def layer(axes, tokens, norm_gain, weights_gen, segment_ids):
    tp, pp = axes["tp"], axes["pp"]
    count, width = tokens.shape
    groups, qrows, f2 = weights_gen.shape
    per = width // f2
    chunks = CHUNKS
    rows = count // chunks
    me = lax.axis_index("pp")
    z = lax.axis_index("tp")

    ring = [(i, (i - 1) % tp) for i in range(tp)]
    first = cut(tokens, 0, rows)
    rest, first = lax.optimization_barrier((tokens, first))
    step = [first] + [rest[c * rows : (c + 1) * rows] for c in range(1, chunks)]
    got = []
    for k in range(1, tp):
        step = [lax.ppermute(step[c], "tp", ring) for c in range(chunks)]
        got.append(step)

    flat = weights_gen.reshape(groups * qrows, f2)
    part = flat.shape[0] // 2

    def swap(x, mask):
        return lax.ppermute(x, "pp", [(i, i ^ mask) for i in range(pp)])

    def half_of(h):
        return cut(flat, h * part, part)

    slices = {0: [half_of(h) for h in range(2)]}
    order = sorted(range(2, pp, 2), key=lambda m: (bin(m).count("1"), m))
    for m in order:
        bits = [1 << b for b in range(pp.bit_length()) if m >> b & 1]
        via = [bits[0], bits[-1]]
        slices[m] = [swap(slices[m ^ via[h]][h], via[h]) for h in range(2)]
    for m in [0] + order:
        slices[m | 1] = [swap(s, 1) for s in slices[m]]

    floats = rest.astype(F32)
    small = jnp.concatenate([jnp.sum(floats * floats, axis=1), norm_gain.astype(F32)])
    small = small.reshape(-1, 128)
    smalls = [small]
    for k in range(1, tp):
        smalls.append(lax.ppermute(smalls[-1], "tp", ring))
    smalls = [s.reshape(-1) for s in smalls]
    square = sum(s[:count] for s in smalls) / (tp * width)
    inv = lax.rsqrt(square + 1e-05)[:, None]
    gains = jnp.stack([s[count:] for s in smalls])
    which = (z + jnp.arange(tp, dtype=jnp.int32)) % tp
    far = (me ^ (pp - 2)) // per
    step_far = (far - z) % tp
    half_steps = tp // 2
    near = jnp.arange(half_steps, dtype=jnp.int32)
    units1 = jnp.concatenate([near, which[:half_steps], near != step_far]).astype(jnp.int32)
    late_steps = jnp.arange(half_steps, tp - 1, dtype=jnp.int32)
    waits = step_far < half_steps
    early_far = jnp.where(waits, step_far, 0)[None]
    units2 = jnp.concatenate(
        [early_far, late_steps, (z + early_far) % tp, which[half_steps : tp - 1], waits[None], late_steps >= 0]
    ).astype(jnp.int32)

    seg = segment_ids[0]
    begin = jnp.sum((seg[None, :] < seg[:, None]).astype(jnp.int32), axis=1)
    positions = jnp.arange(count, dtype=jnp.int32) - begin
    half = DH // 2
    freq = jnp.exp(jnp.arange(half, dtype=F32) * (-2.0 * math.log(rope_base) / DH))
    angle = freq[:, None] * positions.astype(F32)[None, :]
    cos, sin = jnp.cos(angle), jnp.sin(angle)

    levels = range(max(bin(m).count("1") for m in order) + 1)
    stages = []
    for n in levels:
        here = [m for m in [0] + order if bin(m).count("1") == n]
        if n == 0:
            stages.append([(m | b, h) for m in here for b in range(2) for h in range(2)])
        elif n < levels[-1]:
            stages += [[(m | b, h) for m in here for b in range(2)] for h in range(2)]
        else:
            stages += [[(m | b, h) for m in here for h in range(2)] for b in range(2)]
    state = None
    xs = None
    acc = None
    for n, stage in enumerate(stages):
        masks = sorted({m for m, _ in stage})
        items = [(masks.index(m), h * part, slices[m][h]) for m, h in stage]
        where = jnp.concatenate([me[None], me ^ jnp.array(masks, jnp.int32)]).astype(jnp.int32)
        if n == len(stages) - 2:
            xs = prep(0, 0, tokens, inv, gains, None)
            for k in range(1, half_steps):
                for c in range(chunks):
                    xs = prep(k, c * rows, got[k - 1][c], inv, gains, xs)
            xs, cos, sin, inv, gains, units1, units2, which = lax.optimization_barrier(
                (xs, cos, sin, inv, gains, units1, units2, which)
            )
            acc = early(half_steps, units1, xs, state[0], per, None)
        state = place(state, where, items, groups * qrows, groups, pp)
    whole, weights_rows = state
    for k in range(half_steps, tp - 1):
        for c in range(chunks):
            xs = prep(k, c * rows, got[k - 1][c], inv, gains, xs)
    acc = early(tp - half_steps, units2, xs, whole, per, acc)

    out, past = None, []
    for c in range(chunks):
        near = [kv for at, kv in past if at + rows > c * rows - SPAN + 1]
        out, k, v = late(
            c * rows, which[tp - 1 :], got[-1][c], inv, gains, whole, per, acc, cos, sin,
            begin[None, :], near, out,
        )
        past.append((c * rows, (k, v)))
    return weights_rows, out


def solution(mesh):
    in_specs = (P("pp", "tp"), P("tp"), P("tp", None, "pp"), P("pp", None))
    out_specs = (P("tp", "pp", None), P("pp", "tp"))
    axes = dict(mesh.shape)
    body = functools.partial(shards, axes)
    return jax.shard_map(body, mesh=mesh, in_specs=in_specs, out_specs=out_specs, check_vma=False)
```

```python
import functools
import math

import jax
import jax.numpy as jnp
from jax import lax
from jax.experimental import pallas as pl
from jax.experimental.pallas import tpu as pltpu
from jax.sharding import PartitionSpec as P


DH = 128
GROUP = 8
SPAN = 512
PAIR = 2 * DH
CHUNKS = 4
BF16 = jnp.bfloat16
F32 = jnp.float32

rope_base = 500000.0


NT = (((1,), (1,)), ((), ()))
NN = (((1,), (0,)), ((), ()))


def dot(a, b, dims):
    return lax.dot_general(a, b, dims, preferred_element_type=F32)


def params(mib=56):
    return pltpu.CompilerParams(vmem_limit_bytes=mib << 20)


def any_spec():
    return pl.BlockSpec(memory_space=pl.ANY)


def normalise(x_ref, inv_ref, gain, rows, start, put):
    step = min(rows, 16)

    @pl.loop(0, rows // step, unroll=4)
    def _(i):
        r = pl.multiple_of(i * step, step)
        x = x_ref[pl.ds(r, step), :].astype(F32)
        y = x * inv_ref[pl.ds(start + r, step), :] * gain
        put(start + r, step, y.astype(BF16))


def place_kernel(pieces, old, groups, slices, where_ref, *refs):
    count = len(pieces)
    ins = refs[:count]
    out, rows_out, buf, sem_in, sem_out, sem_rows = refs[count + 2 * old :]
    width = out.shape[2]
    own = out.shape[1] // groups // slices
    me = where_ref[0]
    spots = []
    used = 0
    for which, first, size in pieces:
        spots.append(pl.ds(used, size))
        used += size

    def get(i):
        return pltpu.make_async_copy(ins[i], buf.at[spots[i]], sem_in.at[i])

    def put(i):
        which, first, size = pieces[i]
        at = out.at[where_ref[1 + which], pl.ds(first, size), :]
        return pltpu.make_async_copy(buf.at[spots[i]], at, sem_out.at[i])

    def each(i, act):
        which, first, size = pieces[i]
        col = pl.multiple_of(where_ref[1 + which] * width, width)
        for g in range(groups):
            low, high = g * own * slices, (g + 1) * own * slices
            if high <= first or low >= first + size:
                continue
            at = low + me * own - first

            def go(at=at, col=col, g=g):
                src = buf.at[pl.ds(pl.multiple_of(spots[i].start + at, own), own), :]
                act(pltpu.make_async_copy(src, rows_out.at[g, :, pl.ds(col, width)], sem_rows.at[i, g]))

            if first <= low and high <= first + size:
                go()
            else:
                pl.when((at >= 0) & (at < size))(go)

    for i in range(count):
        get(i).start()
    for i in range(count):
        get(i).wait()
        put(i).start()
        each(i, lambda copy: copy.start())
    for i in range(count):
        put(i).wait()
        each(i, lambda copy: copy.wait())


def place(state, where, items, rows, groups, slices):
    arrays = [x for _, _, x in items]
    pieces = [(which, first, x.shape[0]) for which, first, x in items]
    width = arrays[0].shape[1]
    count = len(arrays)
    total = sum(size for _, _, size in pieces)
    old = 0 if state is None else 1
    grid = pltpu.PrefetchScalarGridSpec(
        num_scalar_prefetch=1,
        grid=(1,),
        in_specs=[any_spec()] * (count + 2 * old),
        out_specs=[any_spec()] * 2,
        scratch_shapes=[
            pltpu.VMEM((total, width), BF16),
            pltpu.SemaphoreType.DMA((count,)),
            pltpu.SemaphoreType.DMA((count,)),
            pltpu.SemaphoreType.DMA((count, groups)),
        ],
    )
    size = total * width * 2
    return pl.pallas_call(
        functools.partial(place_kernel, pieces, old, groups, slices),
        grid_spec=grid,
        out_shape=(
            jax.ShapeDtypeStruct((slices, rows, width), BF16),
            jax.ShapeDtypeStruct((groups, rows // groups // slices, slices * width), BF16),
        ),
        input_output_aliases={count + 1: 0, count + 2: 1} if old else {},
        compiler_params=params(),
        cost_estimate=pl.CostEstimate(flops=size * 100, bytes_accessed=2 * size, transcendentals=0),
        name="place",
    )(where, *arrays, *(state if old else ()))


def prep_kernel(k, x_ref, inv_ref, gain_ref, *refs):
    o_ref = refs[-1]

    def put(r, n, y):
        o_ref[0, pl.ds(r, n), :] = y

    normalise(x_ref, inv_ref, gain_ref[k : k + 1, :], x_ref.shape[0], 0, put)


def prep(k, start, x, inv, gains, out):
    rows, width = x.shape
    block = min(rows, 256)
    at = start // block
    extra = 0 if out is None else 1
    return pl.pallas_call(
        functools.partial(prep_kernel, k),
        grid=(rows // block,),
        in_specs=[
            pl.BlockSpec((block, width), lambda i: (i, 0)),
            pl.BlockSpec((block, 1), lambda i: (at + i, 0)),
            pl.BlockSpec(gains.shape, lambda i: (0, 0)),
        ]
        + [any_spec()] * extra,
        out_specs=pl.BlockSpec((1, block, width), lambda i: (k, at + i, 0)),
        out_shape=jax.ShapeDtypeStruct((gains.shape[0] - 1, inv.shape[0], width), BF16),
        input_output_aliases={3: 0} if extra else {},
        compiler_params=params(),
        cost_estimate=pl.CostEstimate(flops=rows * width * 100, bytes_accessed=rows * width * 4, transcendentals=0),
        name="prep",
    )(x, inv, gains, *([out] if extra else []))


def early_kernel(units, per, old, which_ref, x_hbm, *refs):
    weights = refs[:units]
    acc_ref, xs, sems = refs[-3:]
    _, count, width = xs.shape
    f2 = width // per
    block = min(count, 512)
    first = pl.program_id(0) == 0

    def get(u, i):
        at = pl.ds(pl.multiple_of(i * block, block), block)
        return pltpu.make_async_copy(x_hbm.at[which_ref[u], at], xs.at[u, at], sems.at[u, i])

    @pl.when(first)
    def _():
        for i in range(count // block):
            for u in range(units):
                get(u, i).start()

    @pl.loop(0, count // block)
    def _(i):
        r = pl.ds(pl.multiple_of(i * block, block), block)

        @pl.when(first)
        def _():
            for u in range(units):
                get(u, i).wait()

        if old:
            acc_ref[:, r] = refs[units][:, r]
        else:
            acc_ref[:, r] = jnp.zeros((acc_ref.shape[0], block), F32)
        for u in range(units):

            @pl.when(which_ref[2 * units + u * (count // block) + i] != 0)
            def _():
                total = acc_ref[:, r]
                for j in range(per):
                    total = total + dot(weights[u][0, j], xs[u, r, j * f2 : (j + 1) * f2], NT)
                acc_ref[:, r] = total


def early(units, which, xs, whole, per, acc):
    _, count, width = xs.shape
    rows = whole.shape[1]
    w4 = whole.reshape(-1, per, rows, whole.shape[2])
    block = 2 * PAIR if rows % (2 * PAIR) == 0 else PAIR
    old = 0 if acc is None else 1

    def wspec(u):
        return pl.BlockSpec((1, per, block, whole.shape[2]), lambda n, f: (f[units + u], 0, n, 0))

    aspec = pl.BlockSpec((block, count), lambda n, f: (n, 0))
    grid = pltpu.PrefetchScalarGridSpec(
        num_scalar_prefetch=1,
        grid=(rows // block,),
        in_specs=[any_spec()] + [wspec(u) for u in range(units)] + [aspec] * old,
        out_specs=aspec,
        scratch_shapes=[
            pltpu.VMEM((units, count, width), BF16),
            pltpu.SemaphoreType.DMA((units, count // min(count, 512))),
        ],
    )
    return pl.pallas_call(
        functools.partial(early_kernel, units, per, old),
        grid_spec=grid,
        out_shape=jax.ShapeDtypeStruct((rows, count), F32),
        input_output_aliases={2 + units: 0} if old else {},
        compiler_params=params(60),
        cost_estimate=pl.CostEstimate(
            flops=2 * count * width * units * rows,
            bytes_accessed=units * width * (rows + count) * 2 + count * rows * 4 * (1 + old),
            transcendentals=0,
        ),
        name="early",
    )(which, xs, *([w4] * units), *([acc] if old else []))


def late_kernel(start, sizes, per, groups, aliased, which_ref, inv_ref, gain_ref, cos_ref, sin_ref, begin_ref, *refs):
    hist = len(sizes)
    keys = refs[:hist]
    values = refs[hist : 2 * hist]
    x_hbm, w_hbm, acc_hbm = refs[2 * hist : 2 * hist + 3]
    out_ref, k_ref, v_ref, x_ref, w_ref, acc_ref, xn, bias, kall, vall, sems = refs[2 * hist + 3 + aliased :]
    rows, width = x_ref.shape
    f2 = width // per
    half = DH // 2
    blocks = GROUP // 2 + 1
    span = blocks * PAIR
    before = sum(sizes)
    wide = before + rows
    edges = [sum(sizes[:p]) for p in range(hist + 1)] + [wide]

    def get_x():
        return pltpu.make_async_copy(x_hbm, x_ref, sems.at[0])

    def get_acc(g):
        at = pl.ds(pl.multiple_of(g * span, PAIR), span)
        src = acc_hbm.at[at, pl.ds(start, rows)]
        return pltpu.make_async_copy(src, acc_ref.at[at], sems.at[1 + g])

    def get_w(g, j):
        at = pl.ds(pl.multiple_of(g * span, PAIR), span)
        src = w_hbm.at[which_ref[0], j, at]
        return pltpu.make_async_copy(src, w_ref.at[j, at], sems.at[1 + groups + g * per + j])

    get_x().start()
    for g in range(groups):
        for j in range(per):
            get_w(g, j).start()
        get_acc(g).start()

    key = start - before + lax.broadcasted_iota(jnp.int32, (wide, rows), 0)
    tok = start + lax.broadcasted_iota(jnp.int32, (wide, rows), 1)
    bias[...] = jnp.where((key <= tok) & (key >= begin_ref[...]), 0.0, -1e30)
    last = gain_ref.shape[0] - 1

    def put(r, m, y):
        xn[pl.ds(r, m), :] = y

    get_x().wait()
    normalise(x_ref, inv_ref, gain_ref[last : last + 1, :], rows, 0, put)

    def rotary(u):
        a, b = u[:half], u[half:]
        c, s = cos_ref[...], sin_ref[...]
        return jnp.concatenate([a * c - b * s, b * c + a * s], axis=0)

    for p in range(hist):
        kall[:, edges[p] : edges[p + 1], :] = keys[p][...]
        vall[:, :, edges[p] : edges[p + 1]] = values[p][...]

    def project(at):
        total = acc_ref[at, :]
        for j in range(per):
            total = total + dot(w_ref[j, at, :], xn[:, j * f2 : (j + 1) * f2], NT)
        return total

    @pl.loop(0, groups)
    def _(g):
        for j in range(per):
            get_w(g, j).wait()
        get_acc(g).wait()
        base = g * span
        total = project(pl.ds(pl.multiple_of(base + (blocks - 1) * PAIR, PAIR), PAIR))
        k_ref[g] = rotary(total[:DH]).T.astype(BF16)
        v_ref[g] = total[DH:].astype(BF16)
        kall[g, before:, :] = k_ref[g]
        vall[g, :, before:] = v_ref[g]

        def pair(i):
            return project(pl.ds(pl.multiple_of(base + i * PAIR, PAIR), PAIR))

        def score(total, h):
            q = rotary(total[h * DH : (h + 1) * DH]).astype(BF16)
            s = dot(kall[g], q, NN) * (math.log2(math.e) / math.sqrt(DH))
            return s + bias[...]

        def attend(scores, i, h):
            expo = jnp.exp2(scores - scores.max(axis=0, keepdims=True))
            scale = 1.0 / expo.sum(axis=0, keepdims=True)
            out = dot(vall[g], expo.astype(BF16), NN)
            at = pl.multiple_of((g * (blocks - 1) + i) * PAIR + h * DH, DH)
            out_ref[:, pl.ds(at, DH)] = (out * scale).T.astype(BF16)

        total = pair(0)
        for i in range(blocks - 1):
            scores = [score(total, h) for h in range(2)]
            if i + 1 < blocks - 1:
                total = pair(i + 1)
            for h in range(2):
                attend(scores[h], i, h)


def late(start, which, x, inv, gains, whole, per, acc, cos, sin, begin, past, out):
    rows, width = x.shape
    cols, count = acc.shape
    c = start // rows
    w4 = whole.reshape(-1, per, cols, whole.shape[2])
    sizes = tuple(k.shape[1] for k, _ in past)
    groups = cols // DH // (GROUP + 2)
    heads = groups * GROUP
    aliased = 0 if out is None else 1
    wide = sum(sizes) + rows

    grid = pltpu.PrefetchScalarGridSpec(
        num_scalar_prefetch=1,
        grid=(1,),
        in_specs=[
            pl.BlockSpec((rows, 1), lambda n, f: (c, 0)),
            pl.BlockSpec(gains.shape, lambda n, f: (0, 0)),
            pl.BlockSpec((DH // 2, rows), lambda n, f: (0, c)),
            pl.BlockSpec((DH // 2, rows), lambda n, f: (0, c)),
            pl.BlockSpec((1, rows), lambda n, f: (0, c)),
        ]
        + [pl.BlockSpec((groups, r, DH), lambda n, f: (0, 0, 0)) for r in sizes]
        + [pl.BlockSpec((groups, DH, r), lambda n, f: (0, 0, 0)) for r in sizes]
        + [any_spec()] * (3 + aliased),
        out_specs=[
            pl.BlockSpec((rows, heads * DH), lambda n, f: (c, 0)),
            pl.BlockSpec((groups, rows, DH), lambda n, f: (0, 0, 0)),
            pl.BlockSpec((groups, DH, rows), lambda n, f: (0, 0, 0)),
        ],
        scratch_shapes=[
            pltpu.VMEM((rows, width), BF16),
            pltpu.VMEM((per, cols, whole.shape[2]), BF16),
            pltpu.VMEM((cols, rows), F32),
            pltpu.VMEM((rows, width), BF16),
            pltpu.VMEM((wide, rows), F32),
            pltpu.VMEM((groups, wide, DH), BF16),
            pltpu.VMEM((groups, DH, wide), BF16),
            pltpu.SemaphoreType.DMA((1 + groups + groups * per,)),
        ],
    )
    return pl.pallas_call(
        functools.partial(late_kernel, start, sizes, per, groups, aliased),
        grid_spec=grid,
        out_shape=(
            jax.ShapeDtypeStruct((count, heads * DH), BF16),
            jax.ShapeDtypeStruct((groups, rows, DH), BF16),
            jax.ShapeDtypeStruct((groups, DH, rows), BF16),
        ),
        input_output_aliases={9 + 2 * len(sizes): 0} if aliased else {},
        compiler_params=params(),
        cost_estimate=pl.CostEstimate(
            flops=2 * rows * width * cols + 4 * rows * wide * DH * heads,
            bytes_accessed=width * cols * 2 + rows * cols * 4 + rows * heads * DH * 2,
            transcendentals=rows * wide * heads,
        ),
        name="late",
    )(
        which, inv, gains, cos, sin, begin,
        *[k for k, _ in past], *[v for _, v in past], x, w4, acc, *([out] if aliased else []),
    )


def cut_kernel(first, size, x_hbm, o_ref, sem):
    copy = pltpu.make_async_copy(x_hbm.at[pl.ds(first, size)], o_ref, sem)
    copy.start()
    copy.wait()


def cut(x, first, size):
    return pl.pallas_call(
        functools.partial(cut_kernel, first, size),
        in_specs=[any_spec()],
        out_specs=pl.BlockSpec(memory_space=pltpu.VMEM),
        out_shape=jax.ShapeDtypeStruct((size, x.shape[1]), x.dtype),
        scratch_shapes=[pltpu.SemaphoreType.DMA],
        compiler_params=params(60),
        name="cut",
    )(x)


def shards(axes, tokens, norm_gain, weights_gen, segment_ids):
    return layer(axes, tokens, norm_gain, weights_gen, segment_ids)


def layer(axes, tokens, norm_gain, weights_gen, segment_ids):
    tp, pp = axes["tp"], axes["pp"]
    count, width = tokens.shape
    groups, qrows, f2 = weights_gen.shape
    per = width // f2
    chunks = CHUNKS
    rows = count // chunks
    me = lax.axis_index("pp")
    z = lax.axis_index("tp")

    ring = [(i, (i - 1) % tp) for i in range(tp)]
    first = cut(tokens, 0, rows)
    rest, first = lax.optimization_barrier((tokens, first))
    step = [first] + [rest[c * rows : (c + 1) * rows] for c in range(1, chunks)]
    got = []
    for k in range(1, tp):
        step = [lax.ppermute(step[c], "tp", ring) for c in range(chunks)]
        got.append(step)

    flat = weights_gen.reshape(groups * qrows, f2)
    part = flat.shape[0] // 2

    def swap(x, mask):
        return lax.ppermute(x, "pp", [(i, i ^ mask) for i in range(pp)])

    def half_of(h):
        return cut(flat, h * part, part)

    slices = {0: [half_of(h) for h in range(2)]}
    order = sorted(range(2, pp, 2), key=lambda m: (bin(m).count("1"), m))
    for m in order:
        bits = [1 << b for b in range(pp.bit_length()) if m >> b & 1]
        via = [bits[0], bits[-1]]
        slices[m] = [swap(slices[m ^ via[h]][h], via[h]) for h in range(2)]
    for m in [0] + order:
        slices[m | 1] = [swap(s, 1) for s in slices[m]]

    floats = rest.astype(F32)
    small = jnp.concatenate([jnp.sum(floats * floats, axis=1), norm_gain.astype(F32)])
    small = small.reshape(-1, 128)
    smalls = [small]
    for k in range(1, tp):
        smalls.append(lax.ppermute(smalls[-1], "tp", ring))
    smalls = [s.reshape(-1) for s in smalls]
    square = sum(s[:count] for s in smalls) / (tp * width)
    inv = lax.rsqrt(square + 1e-05)[:, None]
    gains = jnp.stack([s[count:] for s in smalls])
    which = (z + jnp.arange(tp, dtype=jnp.int32)) % tp
    far = (me ^ (pp - 2)) // per
    step_far = (far - z) % tp
    half_steps = tp // 2
    blocks = count // min(count, 512)
    block = jnp.arange(blocks, dtype=jnp.int32)[None, :]
    near = jnp.arange(half_steps, dtype=jnp.int32)
    is_far = near == step_far
    steps1 = jnp.where(is_far, half_steps, near)
    flags1 = ~is_far[:, None] | (block < blocks // 2)
    rest_steps = jnp.arange(half_steps, tp - 1, dtype=jnp.int32)
    waits = step_far < half_steps
    steps2 = jnp.concatenate([jnp.where(waits, step_far, 0)[None], rest_steps])
    flags2 = ~waits | (rest_steps != half_steps)[:, None] | (block >= blocks // 2)
    flags2 = jnp.concatenate([jnp.broadcast_to(waits, (1, blocks)), flags2])
    units1 = jnp.concatenate([steps1, (z + steps1) % tp, flags1.reshape(-1)]).astype(jnp.int32)
    units2 = jnp.concatenate([steps2, (z + steps2) % tp, flags2.reshape(-1)]).astype(jnp.int32)

    seg = segment_ids[0]
    begin = jnp.sum((seg[None, :] < seg[:, None]).astype(jnp.int32), axis=1)
    positions = jnp.arange(count, dtype=jnp.int32) - begin
    half = DH // 2
    freq = jnp.exp(jnp.arange(half, dtype=F32) * (-2.0 * math.log(rope_base) / DH))
    angle = freq[:, None] * positions.astype(F32)[None, :]
    cos, sin = jnp.cos(angle), jnp.sin(angle)

    levels = range(max(bin(m).count("1") for m in order) + 1)
    stages = []
    for n in levels:
        here = [m for m in [0] + order if bin(m).count("1") == n]
        if n == 0:
            stages.append([(m | b, h) for m in here for b in range(2) for h in range(2)])
        elif n < levels[-1]:
            stages += [[(m | b, h) for m in here for b in range(2)] for h in range(2)]
        else:
            stages += [[(m | b, h) for m in here for h in range(2)] for b in range(2)]
    state = None
    xs = None
    acc = None
    for n, stage in enumerate(stages):
        masks = sorted({m for m, _ in stage})
        items = [(masks.index(m), h * part, slices[m][h]) for m, h in stage]
        where = jnp.concatenate([me[None], me ^ jnp.array(masks, jnp.int32)]).astype(jnp.int32)
        if n == len(stages) - 2:
            xs = prep(0, 0, tokens, inv, gains, None)
            for k in range(1, half_steps + 1):
                for c in range(chunks if k < half_steps else chunks // 2):
                    xs = prep(k, c * rows, got[k - 1][c], inv, gains, xs)
            xs, cos, sin, inv, gains, units1, units2, which = lax.optimization_barrier(
                (xs, cos, sin, inv, gains, units1, units2, which)
            )
            acc = early(half_steps, units1, xs, state[0], per, None)
        state = place(state, where, items, groups * qrows, groups, pp)
    whole, weights_rows = state
    for k in range(half_steps, tp - 1):
        for c in range(chunks // 2 if k == half_steps else 0, chunks):
            xs = prep(k, c * rows, got[k - 1][c], inv, gains, xs)
    acc = early(tp - half_steps, units2, xs, whole, per, acc)

    out, past = None, []
    for c in range(chunks):
        near = [kv for at, kv in past if at + rows > c * rows - SPAN + 1]
        out, k, v = late(
            c * rows, which[tp - 1 :], got[-1][c], inv, gains, whole, per, acc, cos, sin,
            begin[None, :], near, out,
        )
        past.append((c * rows, (k, v)))
    return weights_rows, out


def solution(mesh):
    in_specs = (P("pp", "tp"), P("tp"), P("tp", None, "pp"), P("pp", None))
    out_specs = (P("tp", "pp", None), P("pp", "tp"))
    axes = dict(mesh.shape)
    body = functools.partial(shards, axes)
    return jax.shard_map(body, mesh=mesh, in_specs=in_specs, out_specs=out_specs, check_vma=False)
```

```python
import functools
import math

import jax
import jax.numpy as jnp
from jax import lax
from jax.experimental import pallas as pl
from jax.experimental.pallas import tpu as pltpu
from jax.sharding import PartitionSpec as P


DH = 128
GROUP = 8
SPAN = 512
PAIR = 2 * DH
CHUNKS = 4
BF16 = jnp.bfloat16
F32 = jnp.float32

rope_base = 500000.0


NT = (((1,), (1,)), ((), ()))
NN = (((1,), (0,)), ((), ()))


def dot(a, b, dims):
    return lax.dot_general(a, b, dims, preferred_element_type=F32)


def params(mib=63):
    return pltpu.CompilerParams(vmem_limit_bytes=mib << 20)


def any_spec():
    return pl.BlockSpec(memory_space=pl.ANY)


def normalise(x_ref, inv_ref, gain, rows, start, put):
    step = min(rows, 16)

    @pl.loop(0, rows // step, unroll=4)
    def _(i):
        r = pl.multiple_of(i * step, step)
        x = x_ref[pl.ds(r, step), :].astype(F32)
        y = x * inv_ref[pl.ds(start + r, step), :] * gain
        put(start + r, step, y.astype(BF16))


def place_kernel(pieces, cuts, old, groups, slices, where_ref, *refs):
    count = len(pieces)
    ins = refs[:count]
    out, rows_out, buf, sem_in, sem_out, sem_rows = refs[count + 2 * old :]
    width = out.shape[2]
    own = out.shape[1] // groups // slices
    me = where_ref[0]
    spots = []
    used = 0
    for which, first, size in pieces:
        spots.append(pl.ds(used, size))
        used += size

    def get(i, t):
        size = pieces[i][2] // cuts
        src = ins[i].at[pl.ds(t * size, size), :]
        return pltpu.make_async_copy(src, buf.at[pl.ds(spots[i].start + t * size, size)], sem_in.at[i, t])

    def put(i, t):
        which, first, size = pieces[i]
        size = size // cuts
        at = out.at[where_ref[1 + which], pl.ds(first + t * size, size), :]
        return pltpu.make_async_copy(buf.at[pl.ds(spots[i].start + t * size, size)], at, sem_out.at[i, t])

    def each(i, act):
        which, first, size = pieces[i]
        col = pl.multiple_of(where_ref[1 + which] * width, width)
        for g in range(groups):
            low, high = g * own * slices, (g + 1) * own * slices
            if high <= first or low >= first + size:
                continue
            at = low + me * own - first

            def go(at=at, col=col, g=g):
                src = buf.at[pl.ds(pl.multiple_of(spots[i].start + at, own), own), :]
                act(pltpu.make_async_copy(src, rows_out.at[g, :, pl.ds(col, width)], sem_rows.at[i, g]))

            if first <= low and high <= first + size:
                go()
            else:
                pl.when((at >= 0) & (at < size))(go)

    for i in range(count):
        for t in range(cuts):
            get(i, t).start()
    for i in range(count):
        for t in range(cuts):
            get(i, t).wait()
            put(i, t).start()
        each(i, lambda copy: copy.start())
    for i in range(count):
        for t in range(cuts):
            put(i, t).wait()
        each(i, lambda copy: copy.wait())


def place(state, where, items, rows, groups, slices):
    arrays = [x for _, _, x in items]
    pieces = [(which, first, x.shape[0]) for which, first, x in items]
    cuts = 4 if len(items) <= 4 else 2
    width = arrays[0].shape[1]
    count = len(arrays)
    total = sum(size for _, _, size in pieces)
    old = 0 if state is None else 1
    grid = pltpu.PrefetchScalarGridSpec(
        num_scalar_prefetch=1,
        grid=(1,),
        in_specs=[any_spec()] * (count + 2 * old),
        out_specs=[any_spec()] * 2,
        scratch_shapes=[
            pltpu.VMEM((total, width), BF16),
            pltpu.SemaphoreType.DMA((count, cuts)),
            pltpu.SemaphoreType.DMA((count, cuts)),
            pltpu.SemaphoreType.DMA((count, groups)),
        ],
    )
    size = total * width * 2
    return pl.pallas_call(
        functools.partial(place_kernel, pieces, cuts, old, groups, slices),
        grid_spec=grid,
        out_shape=(
            jax.ShapeDtypeStruct((slices, rows, width), BF16),
            jax.ShapeDtypeStruct((groups, rows // groups // slices, slices * width), BF16),
        ),
        input_output_aliases={count + 1: 0, count + 2: 1} if old else {},
        compiler_params=params(),
        cost_estimate=pl.CostEstimate(flops=size * 100, bytes_accessed=2 * size, transcendentals=0),
        name="place",
    )(where, *arrays, *(state if old else ()))


def prep_kernel(k, x_ref, inv_ref, gain_ref, *refs):
    o_ref = refs[-1]

    def put(r, n, y):
        o_ref[0, pl.ds(r, n), :] = y

    normalise(x_ref, inv_ref, gain_ref[k : k + 1, :], x_ref.shape[0], 0, put)


def prep(k, start, x, inv, gains, out):
    rows, width = x.shape
    block = min(rows, 128)
    at = start // block
    extra = 0 if out is None else 1
    return pl.pallas_call(
        functools.partial(prep_kernel, k),
        grid=(rows // block,),
        in_specs=[
            pl.BlockSpec((block, width), lambda i: (i, 0)),
            pl.BlockSpec((block, 1), lambda i: (at + i, 0)),
            pl.BlockSpec(gains.shape, lambda i: (0, 0)),
        ]
        + [any_spec()] * extra,
        out_specs=pl.BlockSpec((1, block, width), lambda i: (k, at + i, 0)),
        out_shape=jax.ShapeDtypeStruct((gains.shape[0] - 1, inv.shape[0], width), BF16),
        input_output_aliases={3: 0} if extra else {},
        compiler_params=params(),
        cost_estimate=pl.CostEstimate(flops=rows * width * 100, bytes_accessed=rows * width * 4, transcendentals=0),
        name="prep",
    )(x, inv, gains, *([out] if extra else []))


def early_kernel(units, per, old, which_ref, x_hbm, *refs):
    weights = refs[:units]
    acc_ref, xs, sems = refs[-3:]
    _, count, width = xs.shape
    f2 = width // per
    block = min(count, 512)
    first = pl.program_id(0) == 0

    def get(u, i):
        at = pl.ds(pl.multiple_of(i * block, block), block)
        return pltpu.make_async_copy(x_hbm.at[which_ref[u], at], xs.at[u, at], sems.at[u, i])

    @pl.when(first)
    def _():
        for i in range(count // block):
            for u in range(units):
                get(u, i).start()

    @pl.loop(0, count // block)
    def _(i):
        r = pl.ds(pl.multiple_of(i * block, block), block)

        @pl.when(first)
        def _():
            for u in range(units):
                get(u, i).wait()

        if old:
            acc_ref[:, r] = refs[units][:, r]
        else:
            acc_ref[:, r] = jnp.zeros((acc_ref.shape[0], block), F32)
        for u in range(units):

            @pl.when(which_ref[2 * units + u * (count // block) + i] != 0)
            def _():
                total = acc_ref[:, r]
                for j in range(per):
                    total = total + dot(weights[u][0, j], xs[u, r, j * f2 : (j + 1) * f2], NT)
                acc_ref[:, r] = total


def early(units, which, xs, whole, per, acc):
    _, count, width = xs.shape
    rows = whole.shape[1]
    w4 = whole.reshape(-1, per, rows, whole.shape[2])
    block = 2 * PAIR if rows % (2 * PAIR) == 0 else PAIR
    old = 0 if acc is None else 1

    def wspec(u):
        return pl.BlockSpec((1, per, block, whole.shape[2]), lambda n, f: (f[units + u], 0, n, 0))

    aspec = pl.BlockSpec((block, count), lambda n, f: (n, 0))
    grid = pltpu.PrefetchScalarGridSpec(
        num_scalar_prefetch=1,
        grid=(rows // block,),
        in_specs=[any_spec()] + [wspec(u) for u in range(units)] + [aspec] * old,
        out_specs=aspec,
        scratch_shapes=[
            pltpu.VMEM((units, count, width), BF16),
            pltpu.SemaphoreType.DMA((units, count // min(count, 512))),
        ],
    )
    return pl.pallas_call(
        functools.partial(early_kernel, units, per, old),
        grid_spec=grid,
        out_shape=jax.ShapeDtypeStruct((rows, count), F32),
        input_output_aliases={2 + units: 0} if old else {},
        compiler_params=params(),
        cost_estimate=pl.CostEstimate(
            flops=2 * count * width * units * rows,
            bytes_accessed=units * width * (rows + count) * 2 + count * rows * 4 * (1 + old),
            transcendentals=0,
        ),
        name="early",
    )(which, xs, *([w4] * units), *([acc] if old else []))


def late_kernel(start, sizes, per, groups, aliased, which_ref, inv_ref, gain_ref, cos_ref, sin_ref, begin_ref, *refs):
    hist = len(sizes)
    keys = refs[:hist]
    values = refs[hist : 2 * hist]
    x_hbm, w_hbm, acc_hbm = refs[2 * hist : 2 * hist + 3]
    out_ref, k_ref, v_ref, x_ref, w_ref, acc_ref, xn, bias, kall, vall, sems = refs[2 * hist + 3 + aliased :]
    rows, width = x_ref.shape
    f2 = width // per
    half = DH // 2
    blocks = GROUP // 2 + 1
    span = blocks * PAIR
    before = sum(sizes)
    wide = before + rows
    edges = [sum(sizes[:p]) for p in range(hist + 1)] + [wide]

    def get_x():
        return pltpu.make_async_copy(x_hbm, x_ref, sems.at[0])

    def get_acc(g):
        at = pl.ds(pl.multiple_of(g * span, PAIR), span)
        src = acc_hbm.at[at, pl.ds(start, rows)]
        return pltpu.make_async_copy(src, acc_ref.at[at], sems.at[1 + g])

    def get_w(g, j):
        at = pl.ds(pl.multiple_of(g * span, PAIR), span)
        src = w_hbm.at[which_ref[0], j, at]
        return pltpu.make_async_copy(src, w_ref.at[j, at], sems.at[1 + groups + g * per + j])

    get_x().start()
    for g in range(groups):
        for j in range(per):
            get_w(g, j).start()
        get_acc(g).start()

    key = start - before + lax.broadcasted_iota(jnp.int32, (wide, rows), 0)
    tok = start + lax.broadcasted_iota(jnp.int32, (wide, rows), 1)
    bias[...] = jnp.where((key <= tok) & (key >= begin_ref[...]), 0.0, -1e30)
    last = gain_ref.shape[0] - 1

    def put(r, m, y):
        xn[pl.ds(r, m), :] = y

    get_x().wait()
    normalise(x_ref, inv_ref, gain_ref[last : last + 1, :], rows, 0, put)

    def rotary(u):
        a, b = u[:half], u[half:]
        c, s = cos_ref[...], sin_ref[...]
        return jnp.concatenate([a * c - b * s, b * c + a * s], axis=0)

    for p in range(hist):
        kall[:, edges[p] : edges[p + 1], :] = keys[p][...]
        vall[:, :, edges[p] : edges[p + 1]] = values[p][...]

    def project(at):
        total = acc_ref[at, :]
        for j in range(per):
            total = total + dot(w_ref[j, at, :], xn[:, j * f2 : (j + 1) * f2], NT)
        return total

    @pl.loop(0, groups)
    def _(g):
        for j in range(per):
            get_w(g, j).wait()
        get_acc(g).wait()
        base = g * span
        total = project(pl.ds(pl.multiple_of(base + (blocks - 1) * PAIR, PAIR), PAIR))
        k_ref[g] = rotary(total[:DH]).T.astype(BF16)
        v_ref[g] = total[DH:].astype(BF16)
        kall[g, before:, :] = k_ref[g]
        vall[g, :, before:] = v_ref[g]

        def pair(i):
            return project(pl.ds(pl.multiple_of(base + i * PAIR, PAIR), PAIR))

        def score(total, h):
            q = rotary(total[h * DH : (h + 1) * DH]).astype(BF16)
            s = dot(kall[g], q, NN) * (math.log2(math.e) / math.sqrt(DH))
            return s + bias[...]

        def attend(scores, i, h):
            expo = jnp.exp2(scores - scores.max(axis=0, keepdims=True))
            scale = 1.0 / expo.sum(axis=0, keepdims=True)
            out = dot(vall[g], expo.astype(BF16), NN)
            at = pl.multiple_of((g * (blocks - 1) + i) * PAIR + h * DH, DH)
            out_ref[:, pl.ds(at, DH)] = (out * scale).T.astype(BF16)

        total = pair(0)
        for i in range(blocks - 1):
            scores = [score(total, h) for h in range(2)]
            if i + 1 < blocks - 1:
                total = pair(i + 1)
            for h in range(2):
                attend(scores[h], i, h)


def late(start, which, x, inv, gains, whole, per, acc, cos, sin, begin, past, out):
    rows, width = x.shape
    cols, count = acc.shape
    c = start // rows
    w4 = whole.reshape(-1, per, cols, whole.shape[2])
    sizes = tuple(k.shape[1] for k, _ in past)
    groups = cols // DH // (GROUP + 2)
    heads = groups * GROUP
    aliased = 0 if out is None else 1
    wide = sum(sizes) + rows

    grid = pltpu.PrefetchScalarGridSpec(
        num_scalar_prefetch=1,
        grid=(1,),
        in_specs=[
            pl.BlockSpec((rows, 1), lambda n, f: (c, 0)),
            pl.BlockSpec(gains.shape, lambda n, f: (0, 0)),
            pl.BlockSpec((DH // 2, rows), lambda n, f: (0, c)),
            pl.BlockSpec((DH // 2, rows), lambda n, f: (0, c)),
            pl.BlockSpec((1, rows), lambda n, f: (0, c)),
        ]
        + [pl.BlockSpec((groups, r, DH), lambda n, f: (0, 0, 0)) for r in sizes]
        + [pl.BlockSpec((groups, DH, r), lambda n, f: (0, 0, 0)) for r in sizes]
        + [any_spec()] * (3 + aliased),
        out_specs=[
            pl.BlockSpec((rows, heads * DH), lambda n, f: (c, 0)),
            pl.BlockSpec((groups, rows, DH), lambda n, f: (0, 0, 0)),
            pl.BlockSpec((groups, DH, rows), lambda n, f: (0, 0, 0)),
        ],
        scratch_shapes=[
            pltpu.VMEM((rows, width), BF16),
            pltpu.VMEM((per, cols, whole.shape[2]), BF16),
            pltpu.VMEM((cols, rows), F32),
            pltpu.VMEM((rows, width), BF16),
            pltpu.VMEM((wide, rows), F32),
            pltpu.VMEM((groups, wide, DH), BF16),
            pltpu.VMEM((groups, DH, wide), BF16),
            pltpu.SemaphoreType.DMA((1 + groups + groups * per,)),
        ],
    )
    return pl.pallas_call(
        functools.partial(late_kernel, start, sizes, per, groups, aliased),
        grid_spec=grid,
        out_shape=(
            jax.ShapeDtypeStruct((count, heads * DH), BF16),
            jax.ShapeDtypeStruct((groups, rows, DH), BF16),
            jax.ShapeDtypeStruct((groups, DH, rows), BF16),
        ),
        input_output_aliases={9 + 2 * len(sizes): 0} if aliased else {},
        compiler_params=params(),
        cost_estimate=pl.CostEstimate(
            flops=2 * rows * width * cols + 4 * rows * wide * DH * heads,
            bytes_accessed=width * cols * 2 + rows * cols * 4 + rows * heads * DH * 2,
            transcendentals=rows * wide * heads,
        ),
        name="late",
    )(
        which, inv, gains, cos, sin, begin,
        *[k for k, _ in past], *[v for _, v in past], x, w4, acc, *([out] if aliased else []),
    )


def cut_kernel(first, size, cuts, x_hbm, o_hbm, buf, sem_in, sem_out):
    step = size // cuts

    def get(t):
        at = pl.ds(t * step, step)
        return pltpu.make_async_copy(x_hbm.at[pl.ds(first + t * step, step)], buf.at[at], sem_in.at[t])

    def put(t):
        at = pl.ds(t * step, step)
        return pltpu.make_async_copy(buf.at[at], o_hbm.at[at], sem_out.at[t])

    for t in range(cuts):
        get(t).start()
    for t in range(cuts):
        get(t).wait()
        put(t).start()
    for t in range(cuts):
        put(t).wait()


def cut(x, first, size):
    cuts = 4
    return pl.pallas_call(
        functools.partial(cut_kernel, first, size, cuts),
        in_specs=[any_spec()],
        out_specs=any_spec(),
        out_shape=jax.ShapeDtypeStruct((size, x.shape[1]), x.dtype),
        scratch_shapes=[
            pltpu.VMEM((size, x.shape[1]), x.dtype),
            pltpu.SemaphoreType.DMA((cuts,)),
            pltpu.SemaphoreType.DMA((cuts,)),
        ],
        compiler_params=params(),
        name="cut",
    )(x)


def shards(axes, tokens, norm_gain, weights_gen, segment_ids):
    return layer(axes, tokens, norm_gain, weights_gen, segment_ids)


def layer(axes, tokens, norm_gain, weights_gen, segment_ids):
    tp, pp = axes["tp"], axes["pp"]
    count, width = tokens.shape
    groups, qrows, f2 = weights_gen.shape
    per = width // f2
    chunks = CHUNKS
    rows = count // chunks
    me = lax.axis_index("pp")
    z = lax.axis_index("tp")

    ring = [(i, (i - 1) % tp) for i in range(tp)]
    first = cut(tokens, 0, rows)
    rest, first = lax.optimization_barrier((tokens, first))
    step = [first] + [rest[c * rows : (c + 1) * rows] for c in range(1, chunks)]
    got = []
    for k in range(1, tp):
        step = [lax.ppermute(step[c], "tp", ring) for c in range(chunks)]
        got.append(step)

    flat = weights_gen.reshape(groups * qrows, f2)
    part = flat.shape[0] // 2

    def swap(x, mask):
        return lax.ppermute(x, "pp", [(i, i ^ mask) for i in range(pp)])

    def half_of(h):
        return cut(flat, h * part, part)

    slices = {0: [half_of(h) for h in range(2)]}
    order = sorted(range(2, pp, 2), key=lambda m: (bin(m).count("1"), m))
    for m in order:
        bits = [1 << b for b in range(pp.bit_length()) if m >> b & 1]
        via = [bits[0], bits[-1]]
        slices[m] = [swap(slices[m ^ via[h]][h], via[h]) for h in range(2)]
    for m in [0] + order:
        slices[m | 1] = [swap(s, 1) for s in slices[m]]

    floats = rest.astype(F32)
    small = jnp.concatenate([jnp.sum(floats * floats, axis=1), norm_gain.astype(F32)])
    small = small.reshape(-1, 128)
    smalls = [small]
    for k in range(1, tp):
        smalls.append(lax.ppermute(smalls[-1], "tp", ring))
    smalls = [s.reshape(-1) for s in smalls]
    square = sum(s[:count] for s in smalls) / (tp * width)
    inv = lax.rsqrt(square + 1e-05)[:, None]
    gains = jnp.stack([s[count:] for s in smalls])
    which = (z + jnp.arange(tp, dtype=jnp.int32)) % tp
    far = (me ^ (pp - 2)) // per
    step_far = (far - z) % tp
    half_steps = tp // 2
    blocks = count // min(count, 512)
    block = jnp.arange(blocks, dtype=jnp.int32)[None, :]
    near = jnp.arange(half_steps, dtype=jnp.int32)
    is_far = near == step_far
    steps1 = jnp.where(is_far, half_steps, near)
    flags1 = ~is_far[:, None] | (block < blocks // 2)
    rest_steps = jnp.arange(half_steps, tp - 1, dtype=jnp.int32)
    waits = step_far < half_steps
    steps2 = jnp.concatenate([jnp.where(waits, step_far, 0)[None], rest_steps])
    flags2 = ~waits | (rest_steps != half_steps)[:, None] | (block >= blocks // 2)
    flags2 = jnp.concatenate([jnp.broadcast_to(waits, (1, blocks)), flags2])
    units1 = jnp.concatenate([steps1, (z + steps1) % tp, flags1.reshape(-1)]).astype(jnp.int32)
    units2 = jnp.concatenate([steps2, (z + steps2) % tp, flags2.reshape(-1)]).astype(jnp.int32)

    seg = segment_ids[0]
    begin = jnp.sum((seg[None, :] < seg[:, None]).astype(jnp.int32), axis=1)
    positions = jnp.arange(count, dtype=jnp.int32) - begin
    half = DH // 2
    freq = jnp.exp(jnp.arange(half, dtype=F32) * (-2.0 * math.log(rope_base) / DH))
    angle = freq[:, None] * positions.astype(F32)[None, :]
    cos, sin = jnp.cos(angle), jnp.sin(angle)

    levels = range(max(bin(m).count("1") for m in order) + 1)
    stages = []
    for n in levels:
        here = [m for m in [0] + order if bin(m).count("1") == n]
        if n == 0:
            stages.append([(m | b, h) for m in here for b in range(2) for h in range(2)])
        elif n < levels[-1]:
            stages += [[(m | b, h) for m in here for b in range(2)] for h in range(2)]
        else:
            stages += [[(m | b, h) for m in here for h in range(2)] for b in range(2)]
    state = None
    xs = None
    acc = None
    for n, stage in enumerate(stages):
        masks = sorted({m for m, _ in stage})
        items = [(masks.index(m), h * part, slices[m][h]) for m, h in stage]
        where = jnp.concatenate([me[None], me ^ jnp.array(masks, jnp.int32)]).astype(jnp.int32)
        if n == len(stages) - 2:
            xs = prep(0, 0, tokens, inv, gains, None)
            for k in range(1, half_steps + 1):
                for c in range(chunks if k < half_steps else chunks // 2):
                    xs = prep(k, c * rows, got[k - 1][c], inv, gains, xs)
            xs, cos, sin, inv, gains, units1, units2, which = lax.optimization_barrier(
                (xs, cos, sin, inv, gains, units1, units2, which)
            )
            acc = early(half_steps, units1, xs, state[0], per, None)
        state = place(state, where, items, groups * qrows, groups, pp)
    whole, weights_rows = state
    for k in range(half_steps, tp - 1):
        for c in range(chunks // 2 if k == half_steps else 0, chunks):
            xs = prep(k, c * rows, got[k - 1][c], inv, gains, xs)
    acc = early(tp - half_steps, units2, xs, whole, per, acc)

    out, past = None, []
    for c in range(chunks):
        near = [kv for at, kv in past if at + rows > c * rows - SPAN + 1]
        out, k, v = late(
            c * rows, which[tp - 1 :], got[-1][c], inv, gains, whole, per, acc, cos, sin,
            begin[None, :], near, out,
        )
        past.append((c * rows, (k, v)))
    return weights_rows, out


def solution(mesh):
    in_specs = (P("pp", "tp"), P("tp"), P("tp", None, "pp"), P("pp", None))
    out_specs = (P("tp", "pp", None), P("pp", "tp"))
    axes = dict(mesh.shape)
    body = functools.partial(shards, axes)
    return jax.shard_map(body, mesh=mesh, in_specs=in_specs, out_specs=out_specs, check_vma=False)
```
